32 devices in a mesh: row: 8 (over y, x, core), col: 4 (over z).
Axes of the slice: x: 2, y: 2, z: 4, core: 2. Of those that a mesh axis runs over, the one named last changes fastest.
Arguments:
- blocks: bfloat16 [8, 4, 368, 128, 128], P('row', 'col'), may hold values from -0.125 to 0.125
- block_rows: int32 [8, 4, 368], P('row', 'col'), may hold values from 0 to 31, as said below
- block_cols: int32 [8, 4, 368], P('row', 'col'), may hold values from 0 to 63
- counts: int32 [8, 4], P('row', 'col'), may hold values from 1 to 368, as said below
- features: bfloat16 [32768, 256], P(('col', 'row')), may hold values from -6 to 6
Outputs:
- aggregated: bfloat16 [32768, 256], P(('row', 'col'))
The draws below stay inside these ranges and needn't reach their ends.
Inputs may be any that keep to these rules, and one draw needn't show every extreme that they name: `block_rows`: within one tile the live slots name distinct pairs of block row and block column. `counts`: some tile holds exactly 368 live blocks in every draw.
All inputs are finite; a program needn't handle non-finite values.
Results may differ from the reference program's by a relative error of at most 0.013.
Values may be sent and summed in bfloat16 or wider, within the bound.
A program may use at most 128 MiB of HBM per device.

```python
import jax
import jax.numpy as jnp
from jax import lax

F = 256
BS = 128
Q = 8
MAXB = 368
BR = 32
BC = 64
NB = 256
NODES = 32768
N_ROW = 8
N_COL = 4


def pattern_draw(key):
    base_key = jax.random.fold_in(key, 7)
    slot_key = jax.random.fold_in(base_key, 1)
    count_key = jax.random.fold_in(base_key, 2)
    chosen_key = jax.random.fold_in(base_key, 3)
    tile_total = N_ROW * N_COL
    tile_keys = jax.random.split(slot_key, tile_total)
    slot_ids = jax.vmap(lambda tile_key: jax.random.permutation(tile_key, BR * BC)[:MAXB])(tile_keys)
    slot_ids = slot_ids.astype(jnp.int32).reshape(N_ROW, N_COL, MAXB)
    raw_draw = jax.random.randint(count_key, (tile_total,), 0, MAXB + 1, dtype=jnp.int32)
    tile_counts = jnp.maximum(raw_draw * raw_draw // MAXB, 1)
    chosen_tile = jax.random.randint(chosen_key, (), 0, tile_total, dtype=jnp.int32)
    tile_counts = jnp.where(jnp.arange(tile_total, dtype=jnp.int32) == chosen_tile, MAXB, tile_counts)
    return (slot_ids // BC, slot_ids % BC, tile_counts.reshape(N_ROW, N_COL).astype(jnp.int32))


def draw_block_rows(key, part):
    return pattern_draw(key)[0]


def draw_block_cols(key, part):
    return pattern_draw(key)[1]


def draw_counts(key, part):
    return pattern_draw(key)[2]


def level_of(stream_key, extent, pieces, smallest, top_value):
    def one(position, shards_of):
        draws = jax.random.uniform(jax.random.fold_in(jax.random.fold_in(stream_key, 6), position), (shards_of,), jnp.float32, smallest / len(pieces), top_value / len(pieces))
        return jnp.repeat(jnp.exp(draws), extent[position] // shards_of).reshape((-1,) + (1,) * (len(extent) - position - 1))

    factor_of = one(*pieces[0])
    for cut in pieces[1:]:
        factor_of = factor_of * one(*cut)
    return factor_of


def noise(key, shape, spread, limit, pieces=(), kind=jnp.bfloat16):
    result = jax.random.normal(key, shape, jnp.float32) * spread
    if len(pieces) > 0:
        result = level_of(key, shape, pieces, -0.22, 0.18) * result
    return jnp.clip(result, min=-limit, max=limit).astype(kind)


def setup_inputs(seed: int = 0) -> dict:
    seeds = jax.random.split(jax.random.key(seed), 6)
    return {
        "blocks": noise(seeds[0], (N_ROW, N_COL, MAXB, BS, BS), (BS * MAXB // (3 * Q)) ** -0.5, 0.125, ((0, 8), (1, 4))),
        "block_rows": draw_block_rows(jax.random.fold_in(seeds[5], 71), 0),
        "block_cols": draw_block_cols(jax.random.fold_in(seeds[5], 71), 0),
        "counts": draw_counts(jax.random.fold_in(seeds[5], 71), 0),
        "features": noise(seeds[4], (NODES, F), 1.0, 6.0, ((0, 32),)),
    }


def reference(blocks, block_rows, block_cols, counts, features):
    feature_blocks = features.reshape(NB, BS, F)

    def per_tile(running, tile_index):
        row_panel = tile_index // N_COL
        col_panel = tile_index % N_COL
        tile_blocks = blocks[row_panel, col_panel]
        tile_rows = block_rows[row_panel, col_panel]
        tile_cols = block_cols[row_panel, col_panel]
        live_mask = jnp.arange(MAXB, dtype=jnp.int32) < counts[row_panel, col_panel]
        gathered = feature_blocks[(col_panel * BC + tile_cols).astype(jnp.int32)]
        product = jnp.einsum("gik,gkf->gif", tile_blocks.astype(jnp.float32), gathered.astype(jnp.float32))
        product = jnp.where(live_mask[:, None, None], product, jnp.float32(0.0))
        partial_value = jnp.zeros((BR, BS, F), jnp.float32).at[tile_rows.astype(jnp.int32)].add(product)
        rounded = lax.optimization_barrier(partial_value.astype(jnp.bfloat16)).astype(jnp.float32)
        start = (row_panel * BR).astype(jnp.int32)
        zero = jnp.int32(0)
        current = lax.dynamic_slice(running, (start, zero, zero), (BR, BS, F))
        running = lax.dynamic_update_slice(running, current + rounded, (start, zero, zero))
        return running, None

    initial = jnp.zeros((NB, BS, F), jnp.float32)
    running, _ = lax.scan(per_tile, initial, jnp.arange(N_ROW * N_COL, dtype=jnp.int32))
    return running.reshape(NB * BS, F).astype(jnp.bfloat16)
```

```python
import functools

import jax
import jax.numpy as jnp
from jax import lax
from jax.experimental import pallas as pl
from jax.experimental.pallas import tpu as pltpu
from jax.sharding import PartitionSpec as P

MESH = pl.DeviceIdType.MESH
LANES = 128
HALF = LANES // 2
QUARTERS = 4
GROUP = 40


def bits_for(extent):
    return max(1, (extent - 1).bit_length())


def round_up(value, unit):
    return -(-value // unit) * unit


def kernel(
    n_row, n_col, row_blocks, slot_bits, col_bits, groups,
    rows_in, cols_in, count, blocks_hbm, features_hbm, out,
    held, feat, gath, panel, sums, parts, rights, lefts, plan_vmem, plan,
    load_sem, ag_send, ag_recv, rs_send, rs_recv,
):
    lands = (rights, lefts)
    slots = held.shape[0] - 1
    owned = feat.shape[0]
    half = owned // 2
    width = plan_vmem.shape[1] - round_up(row_blocks, LANES)
    me = lax.axis_index("row")
    p = lax.axis_index("col")

    take = pltpu.make_async_copy(
        features_hbm.at[:, :, pl.ds(0, LANES)], feat, load_sem.at[0]
    )
    mine = [
        pltpu.make_async_copy(
            features_hbm.at[pl.ds(s * half, half), :, pl.ds(LANES, LANES)],
            gath.at[2 + s, pl.ds(me * half, half)],
            load_sem.at[1 + s],
        )
        for s in range(2)
    ]
    fetch = pltpu.make_async_copy(blocks_hbm, held.at[pl.ds(0, slots)], load_sem.at[3])
    take.start()
    for copy in mine:
        copy.start()
    fetch.start()

    cube = n_row == 8
    core = lax.rem(me, 2)
    if cube:
        x_bit = lax.rem(me // 2, 2)
        y_bit = me // 4
        other = me + 1 - 2 * core
        beside = me + 2 - 4 * x_bit
        above = me + 4 - 8 * y_bit
        across = beside + 4 - 8 * y_bit
        flip = 1 - 2 * core
        mates = [other, beside, above]
    else:
        mates = [lax.rem(me + k, n_row) for k in range(1, n_row)]

    barrier = pltpu.get_barrier_semaphore()
    for mate in mates:
        pl.semaphore_signal(barrier, inc=1, device_id=(mate, p), device_id_type=MESH)

    @pl.when(p > 0)
    def _():
        pl.semaphore_signal(barrier, inc=1, device_id=(me, p - 1), device_id_type=MESH)

    @pl.when(p < n_col - 1)
    def _():
        pl.semaphore_signal(barrier, inc=1, device_id=(me, p + 1), device_id_type=MESH)

    low = lax.broadcasted_iota(jnp.int32, (held.shape[1], LANES), 1) < HALF

    def swap(value):
        return pltpu.roll(value, HALF, axis=1)

    held[slots] = jnp.zeros(held.shape[1:], held.dtype)
    take.wait()

    def pack(k, _):
        even = feat[2 * k].astype(jnp.float32)
        odd = feat[2 * k + 1].astype(jnp.float32)
        gath[0, me * half + k] = jnp.where(low, even, swap(odd)).astype(jnp.bfloat16)
        gath[1, me * half + k] = jnp.where(low, swap(even), odd).astype(jnp.bfloat16)
        return 0

    lax.fori_loop(0, half, pack, 0)

    inner = jnp.logical_and(p > 0, p < n_col - 1)

    @pl.when(inner)
    def _():
        pl.semaphore_wait(barrier, len(mates) + 2)

    @pl.when(jnp.logical_not(inner))
    def _():
        pl.semaphore_wait(barrier, len(mates) + 1)

    def shard_copy(m, shard, target, send, recv):
        where = gath.at[m, pl.ds(shard * half, half)]
        return pltpu.make_async_remote_copy(
            src_ref=where,
            dst_ref=where,
            send_sem=ag_send.at[m, send],
            recv_sem=ag_recv.at[m, recv],
            device_id=(target, p),
            device_id_type=MESH,
        )

    def expand(m, shard):
        if m > 1:
            return

        def spread(k, _):
            both = gath[m, shard * half + k].astype(jnp.float32)
            turned = swap(both)
            panel[shard * owned + 2 * k] = jnp.where(low, both, turned).astype(jnp.bfloat16)
            panel[shard * owned + 2 * k + 1] = jnp.where(low, turned, both).astype(jnp.bfloat16)
            return 0

        lax.fori_loop(0, half, spread, 0)

    if cube:
        def first_sends(m):
            shard_copy(m, me, beside, 0, 0).start()
            shard_copy(m, me, above, 1, 1).start()
            shard_copy(m, me, other, 2, 3).start()

        def forward(m):
            @pl.when(core == 0)
            def _():
                shard_copy(m, above, me, 1, 1).wait_recv()
                shard_copy(m, above, beside, 3, 2).start()
                shard_copy(m, above, other, 5, 5).start()
                shard_copy(m, beside, me, 0, 0).wait_recv()
                shard_copy(m, beside, other, 4, 4).start()

            @pl.when(core == 1)
            def _():
                shard_copy(m, beside, me, 0, 0).wait_recv()
                shard_copy(m, beside, above, 3, 2).start()
                shard_copy(m, beside, other, 4, 4).start()
                shard_copy(m, above, me, 1, 1).wait_recv()
                shard_copy(m, above, other, 5, 5).start()

        def gathered(m):
            expand(m, me)
            expand(m, beside)
            expand(m, above)
            shard_copy(m, other, me, 2, 3).wait_recv()
            expand(m, other)
            shard_copy(m, beside + flip, me, 4, 4).wait_recv()
            expand(m, beside + flip)
            shard_copy(m, above + flip, me, 5, 5).wait_recv()
            expand(m, above + flip)
            shard_copy(m, across, me, 2, 2).wait_recv()
            shard_copy(m, across, other, 6, 6).start()
            expand(m, across)
            shard_copy(m, across + flip, me, 6, 6).wait_recv()
            expand(m, across + flip)

        sends = 7
    else:
        def first_sends(m):
            for k in range(1, n_row):
                shard_copy(m, me, lax.rem(me + k, n_row), k - 1, k - 1).start()

        def forward(m):
            pass

        def gathered(m):
            expand(m, me)
            for k in range(1, n_row):
                shard = lax.rem(me + n_row - k, n_row)
                shard_copy(m, shard, me, k - 1, k - 1).wait_recv()
                expand(m, shard)

        sends = n_row - 1

    def make_plan():
        def iota(shape, axis):
            return lax.broadcasted_iota(jnp.int32, shape, axis)

        def over_lanes(value):
            return jnp.sum(value.astype(jnp.float32), axis=1, keepdims=True).astype(jnp.int32)

        def over_rows(value):
            return jnp.sum(value, axis=0, keepdims=True)

        square = (slots, slots)
        wide = plan_vmem.shape[1] - width
        row = jnp.where(iota((1, slots), 1) < count[0, 0], rows_in[...], row_blocks)
        eye = iota(square, 0) == iota(square, 1)
        row_down = over_lanes(jnp.where(eye, row, 0))
        col_down = over_lanes(jnp.where(eye, cols_in[...], 0))
        ahead = jnp.logical_and(row == row_down, iota(square, 1) < iota(square, 0))
        rank = over_lanes(jnp.where(ahead, 1, 0))
        line = iota((slots, wide), 1)
        here = over_rows(jnp.where(line == row_down, 1, 0))
        pairs = jnp.where(iota((1, wide), 1) < row_blocks, (here + 1) >> 1, 0)
        before = over_lanes(jnp.where(line < row_down, pairs, 0))
        place = jnp.where(row_down < row_blocks, 2 * before + rank, -1)
        spare = (row_blocks << (slot_bits + col_bits)) + (slots << col_bits)
        packed = (row_down << (slot_bits + col_bits)) + (iota((slots, 1), 0) << col_bits) + col_down
        hit = place == iota((slots, width), 1)
        plan_vmem[:, pl.ds(0, width)] = spare + over_rows(jnp.where(hit, packed - spare, 0))
        small = (wide, wide)
        pairs_down = over_lanes(jnp.where(iota(small, 0) == iota(small, 1), pairs, 0))
        upto = over_rows(jnp.where(iota(small, 0) <= iota(small, 1), pairs_down, 0))
        plan_vmem[:, pl.ds(width, wide)] = jnp.where(here > 0, upto - 1, -1)

    to_scalar = pltpu.make_async_copy(plan_vmem, plan, load_sem.at[4])

    def compute(piece, hooks):
        def tile(word):
            col = word & ((1 << col_bits) - 1)
            if piece < 2:
                return panel[col]
            block = lax.rem(col, owned)
            shard = col // owned
            return gath[2 + block // half, shard * half + lax.rem(block, half)]

        def step(pair, carry):
            total, before = carry
            first = plan[0, 2 * pair]
            second = plan[0, 2 * pair + 1]
            row = first >> (slot_bits + col_bits)
            slot = lambda word: (word >> col_bits) & ((1 << slot_bits) - 1)
            left = jnp.concatenate([held[slot(first)], held[slot(second)]], axis=1)
            right = jnp.concatenate([tile(first), tile(second)], axis=0)
            product = jnp.dot(left, right, preferred_element_type=jnp.float32)
            total = jnp.where(row == before, total, 0.0) + product
            sums[pair] = total.astype(jnp.bfloat16)
            return total, row

        def group(g, carry):
            return lax.fori_loop(
                0, GROUP, lambda u, c: step(g * GROUP + u, c), carry, unroll=True
            )

        carry = (jnp.zeros((held.shape[1], LANES), jnp.float32), jnp.int32(-1))
        start = 0
        for stop, hook in hooks + [(groups, None)]:
            carry = lax.fori_loop(start, stop, group, carry)
            if hook is not None:
                hook()
            start = stop

    def row_sum(i):
        at = plan[0, width + i]
        value = sums[jnp.maximum(at, 0)]
        return jnp.where(at >= 0, value, jnp.zeros_like(value))

    def rs_copy(m, side, d, source):
        return pltpu.make_async_remote_copy(
            src_ref=source,
            dst_ref=lands[side].at[m, d],
            send_sem=rs_send.at[m, side, d],
            recv_sem=rs_recv.at[m, side, d],
            device_id=(me, p + 1 - 2 * side),
            device_id_type=MESH,
        )

    def emit(members):
        for k in range(n_col):
            d = jnp.where(p == n_col - 1, k, n_col - 1 - k)
            for m in members:
                def pick(u, _):
                    if m < 2:
                        value = jnp.where(
                            low, row_sum(d * owned + 2 * u), row_sum(d * owned + 2 * u + 1)
                        )
                    else:
                        value = row_sum(d * owned + (m - 2) * half + u)
                    parts[m, d, u] = value
                    return 0

                lax.fori_loop(0, half, pick, 0)

                @pl.when(jnp.logical_and(p == 0, d > 0))
                def _():
                    rs_copy(m, 0, d, parts.at[m, d]).start()

                @pl.when(jnp.logical_and(p == n_col - 1, d < n_col - 1))
                def _():
                    rs_copy(m, 1, d, parts.at[m, d]).start()

    def pass_on(m, side, d):
        land = lands[side]
        rs_copy(m, side, d, land.at[m, d]).wait_recv()

        def add(k, _):
            land[m, d, k] = (
                land[m, d, k].astype(jnp.float32) + parts[m, d, k].astype(jnp.float32)
            ).astype(jnp.bfloat16)
            return 0

        lax.fori_loop(0, half, add, 0)
        rs_copy(m, side, d, land.at[m, d]).start()

    def relay(members):
        near_end = p >= n_col // 2

        def rightward(k, here):
            d = n_col - 1 - k
            if 0 <= k and d > 1:
                @pl.when(jnp.logical_and(jnp.logical_and(p > 0, p < d), here))
                def _():
                    for m in members:
                        pass_on(m, 0, d)

        def leftward(k, here):
            if 0 <= k < n_col - 2:
                @pl.when(jnp.logical_and(jnp.logical_and(p > k, p < n_col - 1), here))
                def _():
                    for m in members:
                        pass_on(m, 1, k)

        for k in range(n_col):
            rightward(k, jnp.logical_not(near_end))
            leftward(k, near_end)
            leftward(k - 1, jnp.logical_not(near_end))
            rightward(k - 1, near_end)

    def finish(members):
        def total(from_left, from_right):
            for m in members:
                if from_left:
                    rs_copy(m, 0, p, rights.at[m, p]).wait_recv()
                if from_right:
                    rs_copy(m, 1, p, lefts.at[m, p]).wait_recv()

            def whole(m, k):
                value = parts[m, p, k].astype(jnp.float32)
                if from_left:
                    value = value + rights[m, p, k].astype(jnp.float32)
                if from_right:
                    value = value + lefts[m, p, k].astype(jnp.float32)
                return value

            def add(k, _):
                if members == (0, 1):
                    first, second = whole(0, k), whole(1, k)
                    at = pl.ds(0, LANES)
                    out[2 * k, :, at] = jnp.where(low, first, swap(second)).astype(jnp.bfloat16)
                    out[2 * k + 1, :, at] = jnp.where(low, swap(first), second).astype(jnp.bfloat16)
                else:
                    for m in members:
                        at = pl.ds(LANES, LANES)
                        out[(m - 2) * half + k, :, at] = whole(m, k).astype(jnp.bfloat16)
                return 0

            lax.fori_loop(0, half, add, 0)

        pl.when(p == 0)(lambda: total(False, True))
        pl.when(p == n_col - 1)(lambda: total(True, False))
        pl.when(jnp.logical_and(p > 0, p < n_col - 1))(lambda: total(True, True))

    def later_1():
        forward(1)
        first_sends(3)

    first_sends(0)
    make_plan()
    to_scalar.start()
    forward(0)
    first_sends(1)
    for copy in mine:
        copy.wait()
    first_sends(2)
    to_scalar.wait()
    gathered(0)
    fetch.wait()
    cut = max(0, groups - 2)
    compute(0, [(cut, later_1)])
    emit((0,))
    forward(2)
    gathered(1)
    compute(1, [(cut, lambda: forward(3))])
    emit((1,))
    relay((0,))
    gathered(2)
    gathered(3)
    compute(2, [])
    emit((2, 3))
    relay((1,))
    finish((0, 1))
    relay((2, 3))
    finish((2,))
    finish((3,))

    for m in range(QUARTERS):
        for k in range(sends):
            shard_copy(m, me, me, k, 0).wait_send()
        for d in range(n_col):
            @pl.when(p < d)
            def _():
                rs_copy(m, 0, d, parts.at[m, d]).wait_send()

            @pl.when(p > d)
            def _():
                rs_copy(m, 1, d, parts.at[m, d]).wait_send()


def on_device(n_row, n_col, blocks, block_rows, block_cols, counts, features):
    nodes, width = features.shape
    slots, size = blocks.shape[2], blocks.shape[-1]
    owned = nodes // size
    half = owned // 2
    row_blocks = n_col * owned
    panel_blocks = n_row * owned
    slot_bits, col_bits = bits_for(slots + 1), bits_for(panel_blocks)
    most = (slots + min(slots, row_blocks)) // 2
    groups = -(-most // GROUP)
    pairs = groups * GROUP
    planned = round_up(2 * pairs, LANES) + round_up(row_blocks, LANES)
    vmem = lambda *lead: pltpu.VMEM((*lead, size, LANES), jnp.bfloat16)
    smem = pl.BlockSpec(memory_space=pltpu.SMEM)
    near = pl.BlockSpec(memory_space=pltpu.VMEM)
    hbm = pl.BlockSpec(memory_space=pl.ANY)
    links = max(7, n_row - 1)
    result = pl.pallas_call(
        functools.partial(kernel, n_row, n_col, row_blocks, slot_bits, col_bits, groups),
        out_shape=jax.ShapeDtypeStruct((owned, size, width), jnp.bfloat16),
        in_specs=[near, near, smem, hbm, hbm],
        out_specs=near,
        scratch_shapes=[
            vmem(slots + 1),
            vmem(owned),
            vmem(QUARTERS, n_row * half),
            vmem(panel_blocks),
            vmem(pairs),
            vmem(QUARTERS, n_col, half),
            vmem(QUARTERS, n_col, half),
            vmem(QUARTERS, n_col, half),
            pltpu.VMEM((1, planned), jnp.int32),
            pltpu.SMEM((1, planned), jnp.int32),
            pltpu.SemaphoreType.DMA((5,)),
            pltpu.SemaphoreType.DMA((QUARTERS, links)),
            pltpu.SemaphoreType.DMA((QUARTERS, links)),
            pltpu.SemaphoreType.DMA((QUARTERS, 2, n_col)),
            pltpu.SemaphoreType.DMA((QUARTERS, 2, n_col)),
        ],
        compiler_params=pltpu.CompilerParams(
            collective_id=0, has_side_effects=True, vmem_limit_bytes=67043328
        ),
    )(
        block_rows.reshape(1, slots),
        block_cols.reshape(1, slots),
        counts,
        blocks.reshape(slots, size, size),
        features.reshape(owned, size, width),
    )
    return result.reshape(nodes, width)


def solution(mesh):
    return jax.shard_map(
        functools.partial(on_device, mesh.shape["row"], mesh.shape["col"]),
        mesh=mesh,
        in_specs=(
            P("row", "col", None, None, None),
            P("row", "col", None),
            P("row", "col", None),
            P("row", "col"),
            P(("col", "row"), None),
        ),
        out_specs=P(("row", "col"), None),
        check_vma=False,
    )
```

```python
import functools

import jax
import jax.numpy as jnp
from jax import lax
from jax.experimental import pallas as pl
from jax.experimental.pallas import tpu as pltpu
from jax.sharding import PartitionSpec as P

MESH = pl.DeviceIdType.MESH
LANES = 128
HALF = LANES // 2
QUARTERS = 4
GROUP = 40


def bits_for(extent):
    return max(1, (extent - 1).bit_length())


def round_up(value, unit):
    return -(-value // unit) * unit


def kernel(
    n_row, n_col, row_blocks, slot_bits, col_bits, groups,
    rows_in, cols_in, count, blocks_hbm, features_hbm, out,
    held, feat, gath, wide, panel, result, sums, parts, rights, lefts, plan_vmem, plan,
    load_sem, ag_send, ag_recv, rs_send, rs_recv,
):
    lands = (rights, lefts)
    slots = held.shape[0] - 1
    owned = feat.shape[0]
    half = owned // 2
    part = half // 2
    width = plan_vmem.shape[1] - round_up(row_blocks, LANES)
    me = lax.axis_index("row")
    p = lax.axis_index("col")

    take = pltpu.make_async_copy(
        features_hbm.at[:, :, pl.ds(0, LANES)], feat, load_sem.at[0]
    )
    mine = [
        pltpu.make_async_copy(
            features_hbm.at[pl.ds(s * half, half), :, pl.ds(LANES, LANES)],
            wide.at[pl.ds(me * owned + s * half, half)],
            load_sem.at[1 + s],
        )
        for s in range(2)
    ]
    fetch = pltpu.make_async_copy(blocks_hbm, held.at[pl.ds(0, slots)], load_sem.at[3])
    take.start()
    for copy in mine:
        copy.start()
    fetch.start()

    cube = n_row == 8
    core = lax.rem(me, 2)
    if cube:
        x_bit = lax.rem(me // 2, 2)
        y_bit = me // 4
        other = me + 1 - 2 * core
        beside = me + 2 - 4 * x_bit
        above = me + 4 - 8 * y_bit
        across = beside + 4 - 8 * y_bit
        flip = 1 - 2 * core
        mates = [other, beside, above]
    else:
        mates = [lax.rem(me + k, n_row) for k in range(1, n_row)]

    barrier = pltpu.get_barrier_semaphore()
    for mate in mates:
        pl.semaphore_signal(barrier, inc=1, device_id=(mate, p), device_id_type=MESH)

    @pl.when(p > 0)
    def _():
        pl.semaphore_signal(barrier, inc=1, device_id=(me, p - 1), device_id_type=MESH)

    @pl.when(p < n_col - 1)
    def _():
        pl.semaphore_signal(barrier, inc=1, device_id=(me, p + 1), device_id_type=MESH)

    low = lax.broadcasted_iota(jnp.int32, (held.shape[1], LANES), 1) < HALF

    def swap(value):
        return pltpu.roll(value, HALF, axis=1)

    held[slots] = jnp.zeros(held.shape[1:], held.dtype)
    take.wait()

    def pack(k, _):
        even = feat[2 * k].astype(jnp.float32)
        odd = feat[2 * k + 1].astype(jnp.float32)
        gath[0, me * half + k] = jnp.where(low, even, swap(odd)).astype(jnp.bfloat16)
        gath[1, me * half + k] = jnp.where(low, swap(even), odd).astype(jnp.bfloat16)
        return 0

    lax.fori_loop(0, half, pack, 0)

    inner = jnp.logical_and(p > 0, p < n_col - 1)

    @pl.when(inner)
    def _():
        pl.semaphore_wait(barrier, len(mates) + 2)

    @pl.when(jnp.logical_not(inner))
    def _():
        pl.semaphore_wait(barrier, len(mates) + 1)

    def shard_of(m, shard, first, count):
        if m < 2:
            return gath.at[m, pl.ds(shard * half + first, count)]
        return wide.at[pl.ds(shard * owned + (m - 2) * half + first, count)]

    def shard_copy(m, shard, target, send, recv, first=0, count=half):
        where = shard_of(m, shard, first, count)
        return pltpu.make_async_remote_copy(
            src_ref=where,
            dst_ref=where,
            send_sem=ag_send.at[m, send],
            recv_sem=ag_recv.at[m, recv],
            device_id=(target, p),
            device_id_type=MESH,
        )

    def expand(m, shard):
        if m > 1:
            return

        def spread(k, _):
            both = gath[m, shard * half + k].astype(jnp.float32)
            turned = swap(both)
            panel[shard * owned + 2 * k] = jnp.where(low, both, turned).astype(jnp.bfloat16)
            panel[shard * owned + 2 * k + 1] = jnp.where(low, turned, both).astype(jnp.bfloat16)
            return 0

        lax.fori_loop(0, half, spread, 0)

    if cube:
        def first_sends(m):
            shard_copy(m, me, beside, 0, 0).start()
            shard_copy(m, me, above, 1, 1).start()

        def own_chip(m):
            shard_copy(m, me, other, 2, 3).start()

        def forward(m):
            shard_copy(m, above, me, 1, 1).wait_recv()
            shard_copy(m, above, beside, 3, 2, 0, part).start()
            shard_copy(m, above, other, 5, 5).start()
            shard_copy(m, beside, me, 0, 0).wait_recv()
            shard_copy(m, beside, above, 7, 7, part, half - part).start()
            shard_copy(m, beside, other, 4, 4).start()

        def cross(m):
            shard_copy(m, across, me, 2, 2, 0, part).wait_recv()
            shard_copy(m, across, me, 7, 7, part, half - part).wait_recv()
            shard_copy(m, across, other, 6, 6).start()

        def gathered(m):
            expand(m, me)
            expand(m, beside)
            expand(m, above)
            shard_copy(m, other, me, 2, 3).wait_recv()
            expand(m, other)
            shard_copy(m, beside + flip, me, 4, 4).wait_recv()
            expand(m, beside + flip)
            shard_copy(m, above + flip, me, 5, 5).wait_recv()
            expand(m, above + flip)
            if m < 2:
                cross(m)
            expand(m, across)
            shard_copy(m, across + flip, me, 6, 6).wait_recv()
            expand(m, across + flip)

        def sent(m):
            for k in (0, 1, 2, 4, 5, 6):
                shard_copy(m, me, me, k, 0).wait_send()
            shard_copy(m, me, me, 3, 0, 0, part).wait_send()
            shard_copy(m, me, me, 7, 0, part, half - part).wait_send()

    else:
        def first_sends(m):
            for k in range(1, n_row):
                shard_copy(m, me, lax.rem(me + k, n_row), k - 1, k - 1).start()

        def own_chip(m):
            pass

        def forward(m):
            pass

        def cross(m):
            pass

        def gathered(m):
            expand(m, me)
            for k in range(1, n_row):
                shard = lax.rem(me + n_row - k, n_row)
                shard_copy(m, shard, me, k - 1, k - 1).wait_recv()
                expand(m, shard)

        def sent(m):
            for k in range(n_row - 1):
                shard_copy(m, me, me, k, 0).wait_send()

    def make_plan():
        def iota(shape, axis):
            return lax.broadcasted_iota(jnp.int32, shape, axis)

        def over_lanes(value):
            return jnp.sum(value.astype(jnp.float32), axis=1, keepdims=True).astype(jnp.int32)

        def over_rows(value):
            return jnp.sum(value, axis=0, keepdims=True)

        square = (slots, slots)
        rest = plan_vmem.shape[1] - width
        row = jnp.where(iota((1, slots), 1) < count[0, 0], rows_in[...], row_blocks)
        eye = iota(square, 0) == iota(square, 1)
        row_down = over_lanes(jnp.where(eye, row, 0))
        col_down = over_lanes(jnp.where(eye, cols_in[...], 0))
        ahead = jnp.logical_and(row == row_down, iota(square, 1) < iota(square, 0))
        rank = over_lanes(jnp.where(ahead, 1, 0))
        line = iota((slots, rest), 1)
        here = over_rows(jnp.where(line == row_down, 1, 0))
        pairs = jnp.where(iota((1, rest), 1) < row_blocks, (here + 1) >> 1, 0)
        before = over_lanes(jnp.where(line < row_down, pairs, 0))
        place = jnp.where(row_down < row_blocks, 2 * before + rank, -1)
        spare = (row_blocks << (slot_bits + col_bits)) + (slots << col_bits)
        packed = (row_down << (slot_bits + col_bits)) + (iota((slots, 1), 0) << col_bits) + col_down
        hit = place == iota((slots, width), 1)
        plan_vmem[:, pl.ds(0, width)] = spare + over_rows(jnp.where(hit, packed - spare, 0))
        small = (rest, rest)
        pairs_down = over_lanes(jnp.where(iota(small, 0) == iota(small, 1), pairs, 0))
        upto = over_rows(jnp.where(iota(small, 0) <= iota(small, 1), pairs_down, 0))
        plan_vmem[:, pl.ds(width, rest)] = jnp.where(here > 0, upto - 1, -1)

    to_scalar = pltpu.make_async_copy(plan_vmem, plan, load_sem.at[4])

    def compute(piece, hooks):
        def tile(word):
            col = word & ((1 << col_bits) - 1)
            return panel[col] if piece < 2 else wide[col]

        def step(pair, carry):
            total, before = carry
            first = plan[0, 2 * pair]
            second = plan[0, 2 * pair + 1]
            row = first >> (slot_bits + col_bits)
            slot = lambda word: (word >> col_bits) & ((1 << slot_bits) - 1)
            left = jnp.concatenate([held[slot(first)], held[slot(second)]], axis=1)
            right = jnp.concatenate([tile(first), tile(second)], axis=0)
            product = jnp.dot(left, right, preferred_element_type=jnp.float32)
            total = jnp.where(row == before, total, 0.0) + product
            sums[pair] = total.astype(jnp.bfloat16)
            return total, row

        def group(g, carry):
            return lax.fori_loop(
                0, GROUP, lambda u, c: step(g * GROUP + u, c), carry, unroll=True
            )

        carry = (jnp.zeros((held.shape[1], LANES), jnp.float32), jnp.int32(-1))
        start = 0
        for stop, hook in hooks + [(groups, None)]:
            carry = lax.fori_loop(start, stop, group, carry)
            if hook is not None:
                hook()
            start = stop

    def row_sum(i):
        at = plan[0, width + i]
        value = sums[jnp.maximum(at, 0)]
        return jnp.where(at >= 0, value, jnp.zeros_like(value))

    def rs_copy(m, side, d, source):
        return pltpu.make_async_remote_copy(
            src_ref=source,
            dst_ref=lands[side].at[m, d],
            send_sem=rs_send.at[m, side, d],
            recv_sem=rs_recv.at[m, side, d],
            device_id=(me, p + 1 - 2 * side),
            device_id_type=MESH,
        )

    def emit(members):
        for k in range(n_col):
            d = jnp.where(p == n_col - 1, k, n_col - 1 - k)
            for m in members:
                def pick(u, _):
                    if m < 2:
                        value = jnp.where(
                            low, row_sum(d * owned + 2 * u), row_sum(d * owned + 2 * u + 1)
                        )
                    else:
                        value = row_sum(d * owned + (m - 2) * half + u)
                    parts[m, d, u] = value
                    return 0

                lax.fori_loop(0, half, pick, 0)

                @pl.when(jnp.logical_and(p == 0, d > 0))
                def _():
                    rs_copy(m, 0, d, parts.at[m, d]).start()

                @pl.when(jnp.logical_and(p == n_col - 1, d < n_col - 1))
                def _():
                    rs_copy(m, 1, d, parts.at[m, d]).start()

    def pass_on(m, side, d):
        land = lands[side]
        rs_copy(m, side, d, land.at[m, d]).wait_recv()

        def add(k, _):
            land[m, d, k] = (
                land[m, d, k].astype(jnp.float32) + parts[m, d, k].astype(jnp.float32)
            ).astype(jnp.bfloat16)
            return 0

        lax.fori_loop(0, half, add, 0)
        rs_copy(m, side, d, land.at[m, d]).start()

    near_end = p >= n_col // 2

    def rightward(m, k, here):
        d = n_col - 1 - k
        if d > 1:
            @pl.when(jnp.logical_and(jnp.logical_and(p > 0, p < d), here))
            def _():
                pass_on(m, 0, d)

    def leftward(m, k, here):
        if k < n_col - 2:
            @pl.when(jnp.logical_and(jnp.logical_and(p > k, p < n_col - 1), here))
            def _():
                pass_on(m, 1, k)

    def primary(m, k):
        rightward(m, k, jnp.logical_not(near_end))
        leftward(m, k, near_end)

    def secondary(m, k):
        leftward(m, k, jnp.logical_not(near_end))
        rightward(m, k, near_end)

    def rest(m):
        secondary(m, 0)
        for k in range(2, n_col):
            primary(m, k)
            secondary(m, k - 1)

    def leave(members):
        if members == (0, 1):
            rows, at = pl.ds(0, owned), pl.ds(0, LANES)
        else:
            rows, at = pl.ds((members[0] - 2) * half, half), pl.ds(LANES, LANES)
        return pltpu.make_async_copy(
            result.at[rows, :, at], out.at[rows, :, at], load_sem.at[5 + members[0]]
        )

    def finish(members):
        def total(from_left, from_right):
            for m in members:
                if from_left:
                    rs_copy(m, 0, p, rights.at[m, p]).wait_recv()
                if from_right:
                    rs_copy(m, 1, p, lefts.at[m, p]).wait_recv()

            def whole(m, k):
                value = parts[m, p, k].astype(jnp.float32)
                if from_left:
                    value = value + rights[m, p, k].astype(jnp.float32)
                if from_right:
                    value = value + lefts[m, p, k].astype(jnp.float32)
                return value

            def add(k, _):
                if members == (0, 1):
                    first, second = whole(0, k), whole(1, k)
                    at = pl.ds(0, LANES)
                    result[2 * k, :, at] = jnp.where(low, first, swap(second)).astype(jnp.bfloat16)
                    result[2 * k + 1, :, at] = jnp.where(low, swap(first), second).astype(jnp.bfloat16)
                else:
                    for m in members:
                        at = pl.ds(LANES, LANES)
                        result[(m - 2) * half + k, :, at] = whole(m, k).astype(jnp.bfloat16)
                return 0

            lax.fori_loop(0, half, add, 0)

        pl.when(p == 0)(lambda: total(False, True))
        pl.when(p == n_col - 1)(lambda: total(True, False))
        pl.when(jnp.logical_and(p > 0, p < n_col - 1))(lambda: total(True, True))
        leave(members).start()

    def late_0():
        forward(1)
        first_sends(3)
        own_chip(3)

    def late_1():
        forward(3)
        primary(0, 0)

    cut = max(0, groups - 2)
    first_sends(0)
    own_chip(0)
    make_plan()
    to_scalar.start()
    forward(0)
    first_sends(1)
    for copy in mine:
        copy.wait()
    first_sends(2)
    to_scalar.wait()
    gathered(0)
    own_chip(1)
    own_chip(2)
    fetch.wait()
    compute(0, [(cut, late_0)])
    emit((0,))
    forward(2)
    gathered(1)
    compute(1, [(cut, late_1), (groups - 1, lambda: cross(2))])
    emit((1,))
    primary(0, 1)
    gathered(2)
    cross(3)
    gathered(3)
    rest(0)
    compute(2, [(groups - 1, lambda: primary(1, 0))])
    emit((2, 3))
    primary(1, 1)
    rest(1)
    finish((0, 1))
    primary(2, 0)
    primary(3, 0)
    primary(2, 1)
    rest(2)
    primary(3, 1)
    rest(3)
    finish((2,))
    finish((3,))
    for members in ((0, 1), (2,), (3,)):
        leave(members).wait()

    for m in range(QUARTERS):
        sent(m)
        for d in range(n_col):
            @pl.when(p < d)
            def _():
                rs_copy(m, 0, d, parts.at[m, d]).wait_send()

            @pl.when(p > d)
            def _():
                rs_copy(m, 1, d, parts.at[m, d]).wait_send()


def on_device(n_row, n_col, blocks, block_rows, block_cols, counts, features):
    nodes, width = features.shape
    slots, size = blocks.shape[2], blocks.shape[-1]
    owned = nodes // size
    half = owned // 2
    row_blocks = n_col * owned
    panel_blocks = n_row * owned
    slot_bits, col_bits = bits_for(slots + 1), bits_for(panel_blocks)
    most = (slots + min(slots, row_blocks)) // 2
    groups = -(-most // GROUP)
    pairs = groups * GROUP
    planned = round_up(2 * pairs, LANES) + round_up(row_blocks, LANES)
    vmem = lambda *lead: pltpu.VMEM((*lead, size, LANES), jnp.bfloat16)
    smem = pl.BlockSpec(memory_space=pltpu.SMEM)
    near = pl.BlockSpec(memory_space=pltpu.VMEM)
    hbm = pl.BlockSpec(memory_space=pl.ANY)
    links = max(8, n_row - 1)
    result = pl.pallas_call(
        functools.partial(kernel, n_row, n_col, row_blocks, slot_bits, col_bits, groups),
        out_shape=jax.ShapeDtypeStruct((owned, size, width), jnp.bfloat16),
        in_specs=[near, near, smem, hbm, hbm],
        out_specs=hbm,
        scratch_shapes=[
            vmem(slots + 1),
            vmem(owned),
            vmem(2, n_row * half),
            vmem(panel_blocks),
            vmem(panel_blocks),
            pltpu.VMEM((owned, size, width), jnp.bfloat16),
            vmem(pairs),
            vmem(QUARTERS, n_col, half),
            vmem(QUARTERS, n_col, half),
            vmem(QUARTERS, n_col, half),
            pltpu.VMEM((1, planned), jnp.int32),
            pltpu.SMEM((1, planned), jnp.int32),
            pltpu.SemaphoreType.DMA((9,)),
            pltpu.SemaphoreType.DMA((QUARTERS, links)),
            pltpu.SemaphoreType.DMA((QUARTERS, links)),
            pltpu.SemaphoreType.DMA((QUARTERS, 2, n_col)),
            pltpu.SemaphoreType.DMA((QUARTERS, 2, n_col)),
        ],
        compiler_params=pltpu.CompilerParams(
            collective_id=0, has_side_effects=True, vmem_limit_bytes=67043328
        ),
    )(
        block_rows.reshape(1, slots),
        block_cols.reshape(1, slots),
        counts,
        blocks.reshape(slots, size, size),
        features.reshape(owned, size, width),
    )
    return result.reshape(nodes, width)


def solution(mesh):
    return jax.shard_map(
        functools.partial(on_device, mesh.shape["row"], mesh.shape["col"]),
        mesh=mesh,
        in_specs=(
            P("row", "col", None, None, None),
            P("row", "col", None),
            P("row", "col", None),
            P("row", "col"),
            P(("col", "row"), None),
        ),
        out_specs=P(("row", "col"), None),
        check_vma=False,
    )
```

```python
import functools

import jax
import jax.numpy as jnp
from jax import lax
from jax.experimental import pallas as pl
from jax.experimental.pallas import tpu as pltpu
from jax.sharding import PartitionSpec as P

MESH = pl.DeviceIdType.MESH
LANES = 128
HALF = LANES // 2
QUARTERS = 4
GROUP = 40


def bits_for(extent):
    return max(1, (extent - 1).bit_length())


def round_up(value, unit):
    return -(-value // unit) * unit


def kernel(
    n_row, n_col, row_blocks, slot_bits, col_bits, groups,
    rows_hbm, cols_hbm, count, blocks_hbm, features_hbm, out,
    held, feat, gath, wide, panel, sums, parts, rights, lefts, slots_in, plan_vmem, plan,
    load_sem, ag_send, ag_recv, rs_send, rs_recv,
):
    lands = (rights, lefts)
    slots = held.shape[0] - 1
    owned = feat.shape[0]
    half = owned // 2
    part = half // 2
    width = plan_vmem.shape[1] - round_up(row_blocks, LANES)
    me = lax.axis_index("row")
    p = lax.axis_index("col")

    take = pltpu.make_async_copy(
        features_hbm.at[:, :, pl.ds(0, LANES)], feat, load_sem.at[0]
    )
    mine = [
        pltpu.make_async_copy(
            features_hbm.at[pl.ds(s * half, half), :, pl.ds(LANES, LANES)],
            wide.at[pl.ds(me * owned + s * half, half)],
            load_sem.at[1 + s],
        )
        for s in range(2)
    ]
    fetch = pltpu.make_async_copy(blocks_hbm, held.at[pl.ds(0, slots)], load_sem.at[3])
    listed = [
        pltpu.make_async_copy(rows_hbm, slots_in.at[0], load_sem.at[5]),
        pltpu.make_async_copy(cols_hbm, slots_in.at[1], load_sem.at[6]),
    ]
    take.start()
    for copy in listed + mine:
        copy.start()
    fetch.start()

    cube = n_row == 8
    core = lax.rem(me, 2)
    if cube:
        x_bit = lax.rem(me // 2, 2)
        y_bit = me // 4
        other = me + 1 - 2 * core
        beside = me + 2 - 4 * x_bit
        above = me + 4 - 8 * y_bit
        across = beside + 4 - 8 * y_bit
        flip = 1 - 2 * core
        mates = [other, beside, above]
    else:
        mates = [lax.rem(me + k, n_row) for k in range(1, n_row)]

    barrier = pltpu.get_barrier_semaphore()
    for mate in mates:
        pl.semaphore_signal(barrier, inc=1, device_id=(mate, p), device_id_type=MESH)

    @pl.when(p > 0)
    def _():
        pl.semaphore_signal(barrier, inc=1, device_id=(me, p - 1), device_id_type=MESH)

    @pl.when(p < n_col - 1)
    def _():
        pl.semaphore_signal(barrier, inc=1, device_id=(me, p + 1), device_id_type=MESH)

    low = lax.broadcasted_iota(jnp.int32, (held.shape[1], LANES), 1) < HALF

    def swap(value):
        return pltpu.roll(value, HALF, axis=1)

    take.wait()

    def pack(m):
        def one(k, _):
            even = feat[2 * k].astype(jnp.float32)
            odd = feat[2 * k + 1].astype(jnp.float32)
            even, odd = (even, swap(odd)) if m == 0 else (swap(even), odd)
            gath[m, me * half + k] = jnp.where(low, even, odd).astype(jnp.bfloat16)
            return 0

        lax.fori_loop(0, half, one, 0)

    pack(0)
    inner = jnp.logical_and(p > 0, p < n_col - 1)

    @pl.when(inner)
    def _():
        pl.semaphore_wait(barrier, len(mates) + 2)

    @pl.when(jnp.logical_not(inner))
    def _():
        pl.semaphore_wait(barrier, len(mates) + 1)

    def shard_of(m, shard, first, count):
        if m < 2:
            return gath.at[m, pl.ds(shard * half + first, count)]
        return wide.at[pl.ds(shard * owned + (m - 2) * half + first, count)]

    def shard_copy(m, shard, target, send, recv, first=0, count=half):
        where = shard_of(m, shard, first, count)
        return pltpu.make_async_remote_copy(
            src_ref=where,
            dst_ref=where,
            send_sem=ag_send.at[m, send],
            recv_sem=ag_recv.at[m, recv],
            device_id=(target, p),
            device_id_type=MESH,
        )

    def expand(m, shard):
        if m > 1:
            return

        def spread(k, _):
            both = gath[m, shard * half + k].astype(jnp.float32)
            turned = swap(both)
            panel[shard * owned + 2 * k] = jnp.where(low, both, turned).astype(jnp.bfloat16)
            panel[shard * owned + 2 * k + 1] = jnp.where(low, turned, both).astype(jnp.bfloat16)
            return 0

        lax.fori_loop(0, half, spread, 0)

    if cube:
        ahead, behind = (0, part), (part, half - part)

        def first_sends(m):
            shard_copy(m, me, above, 1, 1, *ahead).start()
            shard_copy(m, me, beside, 0, 0, *behind).start()
            shard_copy(m, me, above, 9, 9, *behind).start()
            shard_copy(m, me, beside, 8, 8, *ahead).start()

        def own_chip(m):
            shard_copy(m, me, other, 2, 3).start()

        def forward(m):
            shard_copy(m, above, me, 1, 1, *ahead).wait_recv()
            shard_copy(m, above, beside, 3, 2, *ahead).start()
            shard_copy(m, beside, me, 0, 0, *behind).wait_recv()
            shard_copy(m, beside, above, 7, 7, *behind).start()

        def arrived(m):
            shard_copy(m, above, me, 9, 9, *behind).wait_recv()
            shard_copy(m, above, other, 5, 5).start()
            shard_copy(m, beside, me, 8, 8, *ahead).wait_recv()
            shard_copy(m, beside, other, 4, 4).start()

        def cross(m):
            shard_copy(m, across, me, 2, 2, *ahead).wait_recv()
            shard_copy(m, across, me, 7, 7, *behind).wait_recv()
            shard_copy(m, across, other, 6, 6).start()

        def gathered(m):
            expand(m, me)
            if m < 2:
                arrived(m)
            expand(m, beside)
            expand(m, above)
            shard_copy(m, other, me, 2, 3).wait_recv()
            expand(m, other)
            shard_copy(m, beside + flip, me, 4, 4).wait_recv()
            expand(m, beside + flip)
            shard_copy(m, above + flip, me, 5, 5).wait_recv()
            expand(m, above + flip)
            if m < 2:
                cross(m)
            expand(m, across)
            shard_copy(m, across + flip, me, 6, 6).wait_recv()
            expand(m, across + flip)

        def sent(m):
            for k in (2, 4, 5, 6):
                shard_copy(m, me, me, k, 0).wait_send()
            for k in (1, 3, 8):
                shard_copy(m, me, me, k, 0, *ahead).wait_send()
            for k in (0, 7, 9):
                shard_copy(m, me, me, k, 0, *behind).wait_send()

    else:
        def first_sends(m):
            for k in range(1, n_row):
                shard_copy(m, me, lax.rem(me + k, n_row), k - 1, k - 1).start()

        def own_chip(m):
            pass

        def forward(m):
            pass

        def cross(m):
            pass

        def arrived(m):
            pass

        def gathered(m):
            expand(m, me)
            for k in range(1, n_row):
                shard = lax.rem(me + n_row - k, n_row)
                shard_copy(m, shard, me, k - 1, k - 1).wait_recv()
                expand(m, shard)

        def sent(m):
            for k in range(n_row - 1):
                shard_copy(m, me, me, k, 0).wait_send()

    def make_plan():
        def iota(shape, axis):
            return lax.broadcasted_iota(jnp.int32, shape, axis)

        def over_lanes(value):
            return jnp.sum(value.astype(jnp.float32), axis=1, keepdims=True).astype(jnp.int32)

        def over_rows(value):
            return jnp.sum(value, axis=0, keepdims=True)

        square = (slots, slots)
        rest = plan_vmem.shape[1] - width
        row = jnp.where(iota((1, slots), 1) < count[0, 0], slots_in[0], row_blocks)
        eye = iota(square, 0) == iota(square, 1)
        row_down = over_lanes(jnp.where(eye, row, 0))
        col_down = over_lanes(jnp.where(eye, slots_in[1], 0))
        ahead = jnp.logical_and(row == row_down, iota(square, 1) < iota(square, 0))
        rank = over_lanes(jnp.where(ahead, 1, 0))
        line = iota((slots, rest), 1)
        here = over_rows(jnp.where(line == row_down, 1, 0))
        pairs = jnp.where(iota((1, rest), 1) < row_blocks, (here + 1) >> 1, 0)
        before = over_lanes(jnp.where(line < row_down, pairs, 0))
        place = jnp.where(row_down < row_blocks, 2 * before + rank, -1)
        spare = (row_blocks << (slot_bits + col_bits)) + (slots << col_bits)
        packed = (row_down << (slot_bits + col_bits)) + (iota((slots, 1), 0) << col_bits) + col_down
        hit = place == iota((slots, width), 1)
        plan_vmem[:, pl.ds(0, width)] = spare + over_rows(jnp.where(hit, packed - spare, 0))
        small = (rest, rest)
        pairs_down = over_lanes(jnp.where(iota(small, 0) == iota(small, 1), pairs, 0))
        upto = over_rows(jnp.where(iota(small, 0) <= iota(small, 1), pairs_down, 0))
        plan_vmem[:, pl.ds(width, rest)] = jnp.where(here > 0, upto - 1, -1)

    to_scalar = pltpu.make_async_copy(plan_vmem, plan, load_sem.at[4])

    def compute(piece, hooks):
        def tile(word):
            col = word & ((1 << col_bits) - 1)
            return panel[col] if piece < 2 else wide[col]

        def step(pair, carry):
            total, before = carry
            first = plan[0, 2 * pair]
            second = plan[0, 2 * pair + 1]
            row = first >> (slot_bits + col_bits)
            slot = lambda word: (word >> col_bits) & ((1 << slot_bits) - 1)
            left = jnp.concatenate([held[slot(first)], held[slot(second)]], axis=1)
            right = jnp.concatenate([tile(first), tile(second)], axis=0)
            product = jnp.dot(left, right, preferred_element_type=jnp.float32)
            total = jnp.where(row == before, total, 0.0) + product
            sums[pair] = total.astype(jnp.bfloat16)
            return total, row

        def group(g, carry):
            return lax.fori_loop(
                0, GROUP, lambda u, c: step(g * GROUP + u, c), carry, unroll=True
            )

        carry = (jnp.zeros((held.shape[1], LANES), jnp.float32), jnp.int32(-1))
        start = 0
        for stop, hook in hooks + [(groups, None)]:
            carry = lax.fori_loop(start, stop, group, carry)
            if hook is not None:
                hook()
            start = stop

    def row_sum(i):
        at = plan[0, width + i]
        value = sums[jnp.maximum(at, 0)]
        return jnp.where(at >= 0, value, jnp.zeros_like(value))

    def rs_copy(m, side, d, source):
        return pltpu.make_async_remote_copy(
            src_ref=source,
            dst_ref=lands[side].at[m, d],
            send_sem=rs_send.at[m, side, d],
            recv_sem=rs_recv.at[m, side, d],
            device_id=(me, p + 1 - 2 * side),
            device_id_type=MESH,
        )

    def emit(members):
        for k in range(n_col):
            d = jnp.where(p == n_col - 1, k, n_col - 1 - k)
            for m in members:
                def pick(u, _):
                    if m < 2:
                        value = jnp.where(
                            low, row_sum(d * owned + 2 * u), row_sum(d * owned + 2 * u + 1)
                        )
                    else:
                        value = row_sum(d * owned + (m - 2) * half + u)
                    parts[m, d, u] = value
                    return 0

                lax.fori_loop(0, half, pick, 0)

                @pl.when(jnp.logical_and(p == 0, d > 0))
                def _():
                    rs_copy(m, 0, d, parts.at[m, d]).start()

                @pl.when(jnp.logical_and(p == n_col - 1, d < n_col - 1))
                def _():
                    rs_copy(m, 1, d, parts.at[m, d]).start()

    def pass_on(m, side, d):
        land = lands[side]
        rs_copy(m, side, d, land.at[m, d]).wait_recv()

        def add(k, _):
            land[m, d, k] = (
                land[m, d, k].astype(jnp.float32) + parts[m, d, k].astype(jnp.float32)
            ).astype(jnp.bfloat16)
            return 0

        lax.fori_loop(0, half, add, 0)
        rs_copy(m, side, d, land.at[m, d]).start()

    near_end = p >= n_col // 2

    def rightward(m, k, here):
        d = n_col - 1 - k
        if d > 1:
            @pl.when(jnp.logical_and(jnp.logical_and(p > 0, p < d), here))
            def _():
                pass_on(m, 0, d)

    def leftward(m, k, here):
        if k < n_col - 2:
            @pl.when(jnp.logical_and(jnp.logical_and(p > k, p < n_col - 1), here))
            def _():
                pass_on(m, 1, k)

    def primary(m, k):
        rightward(m, k, jnp.logical_not(near_end))
        leftward(m, k, near_end)

    def secondary(m, k):
        leftward(m, k, jnp.logical_not(near_end))
        rightward(m, k, near_end)

    def rest(m):
        secondary(m, 0)
        for k in range(2, n_col):
            primary(m, k)
            secondary(m, k - 1)

    def finish(members):
        def total(from_left, from_right):
            for m in members:
                if from_left:
                    rs_copy(m, 0, p, rights.at[m, p]).wait_recv()
                if from_right:
                    rs_copy(m, 1, p, lefts.at[m, p]).wait_recv()

            def whole(m, k):
                value = parts[m, p, k].astype(jnp.float32)
                if from_left:
                    value = value + rights[m, p, k].astype(jnp.float32)
                if from_right:
                    value = value + lefts[m, p, k].astype(jnp.float32)
                return value

            def add(k, _):
                if members == (0, 1):
                    first, second = whole(0, k), whole(1, k)
                    at = pl.ds(0, LANES)
                    out[2 * k, :, at] = jnp.where(low, first, swap(second)).astype(jnp.bfloat16)
                    out[2 * k + 1, :, at] = jnp.where(low, swap(first), second).astype(jnp.bfloat16)
                else:
                    for m in members:
                        at = pl.ds(LANES, LANES)
                        out[(m - 2) * half + k, :, at] = whole(m, k).astype(jnp.bfloat16)
                return 0

            lax.fori_loop(0, half, add, 0)

        pl.when(p == 0)(lambda: total(False, True))
        pl.when(p == n_col - 1)(lambda: total(True, False))
        pl.when(jnp.logical_and(p > 0, p < n_col - 1))(lambda: total(True, True))

    def late_0():
        forward(1)
        first_sends(3)
        own_chip(3)

    def late_1():
        forward(3)
        arrived(3)
        primary(0, 0)

    cut = max(0, groups - 2)
    first_sends(0)
    own_chip(0)
    for copy in listed:
        copy.wait()
    make_plan()
    to_scalar.start()
    pack(1)
    held[slots] = jnp.zeros(held.shape[1:], held.dtype)
    forward(0)
    first_sends(1)
    for copy in mine:
        copy.wait()
    first_sends(2)
    to_scalar.wait()
    gathered(0)
    own_chip(1)
    own_chip(2)
    fetch.wait()
    compute(0, [(cut, late_0)])
    emit((0,))
    forward(2)
    arrived(2)
    gathered(1)
    compute(1, [(cut, late_1), (groups - 1, lambda: cross(2))])
    emit((1,))
    primary(0, 1)
    gathered(2)
    cross(3)
    gathered(3)
    rest(0)
    compute(2, [(groups - 1, lambda: primary(1, 0))])
    emit((2, 3))
    primary(1, 1)
    rest(1)
    finish((0, 1))
    primary(2, 0)
    primary(3, 0)
    primary(2, 1)
    rest(2)
    primary(3, 1)
    rest(3)
    finish((2,))
    finish((3,))
    for m in range(QUARTERS):
        sent(m)
        for d in range(n_col):
            @pl.when(p < d)
            def _():
                rs_copy(m, 0, d, parts.at[m, d]).wait_send()

            @pl.when(p > d)
            def _():
                rs_copy(m, 1, d, parts.at[m, d]).wait_send()


def on_device(n_row, n_col, blocks, block_rows, block_cols, counts, features):
    nodes, width = features.shape
    slots, size = blocks.shape[2], blocks.shape[-1]
    owned = nodes // size
    half = owned // 2
    row_blocks = n_col * owned
    panel_blocks = n_row * owned
    slot_bits, col_bits = bits_for(slots + 1), bits_for(panel_blocks)
    most = (slots + min(slots, row_blocks)) // 2
    groups = -(-most // GROUP)
    pairs = groups * GROUP
    planned = round_up(2 * pairs, LANES) + round_up(row_blocks, LANES)
    vmem = lambda *lead: pltpu.VMEM((*lead, size, LANES), jnp.bfloat16)
    near = pl.BlockSpec(memory_space=pltpu.VMEM)
    far = lambda value: pltpu.with_memory_space_constraint(value, pltpu.HBM)
    hbm = pl.BlockSpec(memory_space=pltpu.HBM)
    scratch = size * LANES * 2 * (
        slots + 1 + owned + 2 * n_row * half + 2 * panel_blocks + pairs + 3 * QUARTERS * n_col * half
    )
    limit = scratch + (2 << 20)
    links = max(10, n_row - 1)
    result = pl.pallas_call(
        functools.partial(kernel, n_row, n_col, row_blocks, slot_bits, col_bits, groups),
        out_shape=jax.ShapeDtypeStruct((owned, size, width), jnp.bfloat16),
        in_specs=[hbm, hbm, pl.BlockSpec(memory_space=pltpu.SMEM), hbm, hbm],
        out_specs=near,
        scratch_shapes=[
            vmem(slots + 1),
            vmem(owned),
            vmem(2, n_row * half),
            vmem(panel_blocks),
            vmem(panel_blocks),
            vmem(pairs),
            vmem(QUARTERS, n_col, half),
            vmem(QUARTERS, n_col, half),
            vmem(QUARTERS, n_col, half),
            pltpu.VMEM((2, 1, slots), jnp.int32),
            pltpu.VMEM((1, planned), jnp.int32),
            pltpu.SMEM((1, planned), jnp.int32),
            pltpu.SemaphoreType.DMA((9,)),
            pltpu.SemaphoreType.DMA((QUARTERS, links)),
            pltpu.SemaphoreType.DMA((QUARTERS, links)),
            pltpu.SemaphoreType.DMA((QUARTERS, 2, n_col)),
            pltpu.SemaphoreType.DMA((QUARTERS, 2, n_col)),
        ],
        compiler_params=pltpu.CompilerParams(
            collective_id=0, has_side_effects=True, vmem_limit_bytes=limit
        ),
    )(
        far(block_rows.reshape(1, slots)),
        far(block_cols.reshape(1, slots)),
        counts,
        far(blocks.reshape(slots, size, size)),
        far(features.reshape(owned, size, width)),
    )
    return result.reshape(nodes, width)


def solution(mesh):
    return jax.shard_map(
        functools.partial(on_device, mesh.shape["row"], mesh.shape["col"]),
        mesh=mesh,
        in_specs=(
            P("row", "col", None, None, None),
            P("row", "col", None),
            P("row", "col", None),
            P("row", "col"),
            P(("col", "row"), None),
        ),
        out_specs=P(("row", "col"), None),
        check_vma=False,
    )
```
